32 devices in a mesh: dp: 4 (over y, z), sp: 8 (over x, core).
Axes of the slice: x: 4, y: 2, z: 2, core: 2. Of those that a mesh axis runs over, the one named last changes fastest.
The devices are a block of a 4x4x8 slice.
Arguments:
- image_tokens: bfloat16 [64, 1024, 1152], P('dp', 'sp'), parts along dimension 0
- ln1_gain: float32 [2, 1152], replicated
- ln1_shift: float32 [2, 1152], replicated
- w_qkv: bfloat16 [2, 1152, 3, 16, 72], replicated
- b_qkv: float32 [2, 3, 16, 72], replicated
- w_out: bfloat16 [2, 16, 72, 1152], replicated
- b_out: float32 [2, 1152], replicated
- ln2_gain: float32 [2, 1152], replicated
- ln2_shift: float32 [2, 1152], replicated
- w_up: bfloat16 [2, 1152, 4304], replicated
- b_up: float32 [2, 4304], replicated
- w_down: bfloat16 [2, 4304, 1152], replicated
- b_down: float32 [2, 1152], replicated
Outputs:
- output: bfloat16 [64, 1024, 1152], P('dp', 'sp'), parts along dimension 0
There are 4 independent parts. The reference program is written for one: setup_inputs(seed, part) draws one part's arguments, and reference() takes and returns one part's arrays. A program takes and returns all parts, laid end to end along the dimension named above; an argument that names none is the same for every part.
All inputs are finite; a program needn't handle non-finite values.
Results may differ from the reference program's by a relative error of at most 0.0143792.
Values are sent between devices in bfloat16 or wider.
A program may use at most 768 MiB of HBM per device.

```python
import jax
import jax.numpy as jnp
from jax import lax

IMAGES = 16
SEQ_LEN = 1024
WIDTH = 1152
HEADS = 16
HEAD_DIM = 72
MLP_DIM = 4304
LAYERS = 2
LN_EPS = 1e-6


def layer_norm(tokens, ln_gain, ln_shift):
    values = tokens.astype(jnp.float32)
    mean_val = jnp.mean(values, axis=-1, keepdims=True)
    centred = values - mean_val
    var_val = jnp.mean(centred * centred, axis=-1, keepdims=True)
    return (centred * lax.rsqrt(var_val + LN_EPS) * ln_gain + ln_shift).astype(jnp.bfloat16)


def one_head(head_inputs):
    q_head, k_head, v_head = head_inputs
    score_scale = q_head.shape[-1] ** -0.5
    scores = jnp.einsum('bqe,bke->bqk', q_head.astype(jnp.float32), k_head.astype(jnp.float32)) * score_scale
    row_peak = jnp.max(scores, axis=-1, keepdims=True)
    prob_vals = jnp.exp(scores - row_peak)
    row_total = jnp.sum(prob_vals, axis=-1, keepdims=True)
    mixed_vals = jnp.einsum('bqk,bke->bqe', prob_vals.astype(jnp.bfloat16).astype(jnp.float32), v_head.astype(jnp.float32))
    return (mixed_vals / row_total).astype(jnp.bfloat16)


def encoder_layer(hidden, layer_params):
    (ln1_gain, ln1_shift, w_qkv, b_qkv, w_out, b_out, ln2_gain, ln2_shift, w_up, b_up, w_down, b_down) = layer_params
    normed = layer_norm(hidden, ln1_gain, ln1_shift)
    qkv_all = jnp.einsum('bsd,dthe->bsthe', normed.astype(jnp.float32), w_qkv.astype(jnp.float32)) + b_qkv
    per_head = jnp.moveaxis(qkv_all.astype(jnp.bfloat16), 3, 0)
    heads_out = lax.map(one_head, (per_head[:, :, :, 0], per_head[:, :, :, 1], per_head[:, :, :, 2]))
    attn_proj = jnp.einsum('hbse,hed->bsd', heads_out.astype(jnp.float32), w_out.astype(jnp.float32)) + b_out
    mid_state = (hidden.astype(jnp.float32) + attn_proj).astype(jnp.bfloat16)
    normed_two = layer_norm(mid_state, ln2_gain, ln2_shift)
    up_proj = jnp.einsum('bsd,df->bsf', normed_two.astype(jnp.float32), w_up.astype(jnp.float32)) + b_up
    active = jax.nn.gelu(up_proj, approximate=True).astype(jnp.bfloat16)
    down_proj = jnp.einsum('bsf,fd->bsd', active.astype(jnp.float32), w_down.astype(jnp.float32)) + b_down
    return (mid_state.astype(jnp.float32) + down_proj).astype(jnp.bfloat16)


def setup_inputs(seed: int = 0, part: int = 0) -> dict:
    part_key = jax.random.fold_in(jax.random.key(seed), part)
    key_pattern, key_noise = jax.random.split(part_key, 2)
    period = SEQ_LEN // 8
    half_width = WIDTH // 2
    pattern = jax.random.normal(key_pattern, (IMAGES, period, half_width), jnp.float32)
    repeated = jnp.tile(pattern, (1, SEQ_LEN // period, 1))
    noise_part = jax.random.normal(key_noise, (IMAGES, SEQ_LEN, WIDTH - half_width), jnp.float32)
    image_tokens = jnp.concatenate([repeated, noise_part], axis=-1).astype(jnp.bfloat16)
    key_set = jax.random.split(jax.random.key(seed + 1), 14)
    row_scale = jnp.where(jnp.arange(WIDTH) < half_width, 1.0, 0.2)[:, None, None]
    head_shape = (LAYERS, WIDTH, HEADS, HEAD_DIM)
    w_query = 2.0 * WIDTH ** -0.5 * row_scale * jax.random.normal(key_set[0], head_shape, jnp.float32)
    w_key = w_query + 0.1 * WIDTH ** -0.5 * jax.random.normal(key_set[1], head_shape, jnp.float32)
    w_value = WIDTH ** -0.5 * jax.random.normal(key_set[2], head_shape, jnp.float32)
    w_qkv = jnp.stack([w_query, w_key, w_value], axis=2).astype(jnp.bfloat16)
    b_qkv = 0.3 * jax.random.normal(key_set[3], (LAYERS, 3, HEADS, HEAD_DIM), jnp.float32)
    w_out = (1.5 * WIDTH ** -0.5 * jax.random.normal(key_set[4], (LAYERS, HEADS, HEAD_DIM, WIDTH), jnp.float32)).astype(jnp.bfloat16)
    b_out = 0.3 * jax.random.normal(key_set[5], (LAYERS, WIDTH), jnp.float32)
    ln1_gain = 1.0 + 0.2 * jax.random.normal(key_set[6], (LAYERS, WIDTH), jnp.float32)
    ln1_shift = 0.3 * jax.random.normal(key_set[7], (LAYERS, WIDTH), jnp.float32)
    ln2_gain = 1.0 + 0.2 * jax.random.normal(key_set[8], (LAYERS, WIDTH), jnp.float32)
    ln2_shift = 0.3 * jax.random.normal(key_set[9], (LAYERS, WIDTH), jnp.float32)
    w_up = (WIDTH ** -0.5 * jax.random.normal(key_set[10], (LAYERS, WIDTH, MLP_DIM), jnp.float32)).astype(jnp.bfloat16)
    b_up = 0.3 * jax.random.normal(key_set[11], (LAYERS, MLP_DIM), jnp.float32)
    w_down = (0.5 * MLP_DIM ** -0.5 * jax.random.normal(key_set[12], (LAYERS, MLP_DIM, WIDTH), jnp.float32)).astype(jnp.bfloat16)
    b_down = 0.3 * jax.random.normal(key_set[13], (LAYERS, WIDTH), jnp.float32)
    return {'image_tokens': image_tokens, 'ln1_gain': ln1_gain, 'ln1_shift': ln1_shift, 'w_qkv': w_qkv, 'b_qkv': b_qkv, 'w_out': w_out, 'b_out': b_out, 'ln2_gain': ln2_gain, 'ln2_shift': ln2_shift, 'w_up': w_up, 'b_up': b_up, 'w_down': w_down, 'b_down': b_down}


def reference(image_tokens, ln1_gain, ln1_shift, w_qkv, b_qkv, w_out, b_out, ln2_gain, ln2_shift, w_up, b_up, w_down, b_down):
    stacked = (ln1_gain, ln1_shift, w_qkv, b_qkv, w_out, b_out, ln2_gain, ln2_shift, w_up, b_up, w_down, b_down)

    def layer_body(hidden, layer_params):
        return encoder_layer(hidden, layer_params), None

    return lax.scan(layer_body, image_tokens, stacked)[0]
```

```python
import functools
import math

import jax
import jax.numpy as jnp
from jax import lax
from jax.experimental import pallas as pl
from jax.experimental.pallas import tpu as pltpu
from jax.sharding import PartitionSpec as P

LN_EPS = 1e-6
BF16 = jnp.bfloat16
F32 = jnp.float32
NT = (((1,), (1,)), ((), ()))
VMEM_LIMIT = 60 << 20
WINDOW = 256


def layer_norm(values, gain, shift):
    values = values.astype(F32)
    centred = values - jnp.mean(values, axis=-1, keepdims=True)
    var = jnp.mean(centred * centred, axis=-1, keepdims=True)
    return (centred * lax.rsqrt(var + LN_EPS) * gain + shift).astype(BF16)


def whole(shape):
    return pl.BlockSpec(shape, lambda i: (0,) * len(shape), pipeline_mode=pl.Buffered(1))


def layer_of(layer, shape):
    return pl.BlockSpec((None,) + shape, lambda i: (layer,) + (0,) * len(shape), pipeline_mode=pl.Buffered(1))


def qkv_kernel(x_ref, gain_ref, shift_ref, w_ref, bias_ref, out_ref, *, layer, cols):
    row = slice(layer, layer + 1)
    normed = layer_norm(x_ref[...], gain_ref[row, :], shift_ref[row, :])
    n_out = w_ref.shape[0]
    for c in range(0, n_out, cols):
        w = min(cols, n_out - c)
        y = lax.dot_general(normed, w_ref[c:c + w, :], NT, preferred_element_type=F32)
        out_ref[:, c:c + w] = (y + bias_ref[row, c:c + w]).astype(BF16)


def qkv_call(layer, x, gain, shift, w, bias, rows=512, cols=256):
    m, d = x.shape
    n = w.shape[1]
    return pl.pallas_call(
        functools.partial(qkv_kernel, layer=layer, cols=cols),
        grid=(m // rows,),
        name="qkv",
        in_specs=[pl.BlockSpec((rows, d), lambda i: (i, 0)), whole(gain.shape), whole(shift.shape), layer_of(layer, (n, d)), whole(bias.shape)],
        out_specs=pl.BlockSpec((rows, n), lambda i: (i, 0)),
        out_shape=jax.ShapeDtypeStruct((m, n), BF16),
        compiler_params=pltpu.CompilerParams(vmem_limit_bytes=VMEM_LIMIT),
        cost_estimate=pl.CostEstimate(flops=2 * m * d * n, bytes_accessed=2 * (m * d + n * d + m * n), transcendentals=0),
    )(x, gain, shift, w, bias)


def attn_kernel(qkv_ref, out_ref, s0_ref, s1_ref, k0_ref, k1_ref, *, heads, head_dim, rows, unroll):
    seq = qkv_ref.shape[0]
    d = heads * head_dim
    blocks = seq // rows
    score_scale = (head_dim ** -0.5) * math.log2(math.e)
    s_bufs, k_bufs = (s0_ref, s1_ref), (k0_ref, k1_ref)

    def window(h):
        low = h * head_dim
        off = pl.multiple_of(jnp.minimum(low // 128, d // 128 - 2) * 128, 128)
        low = low - off
        lane = lax.broadcasted_iota(jnp.int32, (1, WINDOW), 1)
        return off, (lane >= low) & (lane < low + head_dim)

    def mask_keys(h, k_buf):
        off, mask = window(h)
        k = qkv_ref[:, pl.ds(pl.multiple_of(d + off, 128), WINDOW)]
        k_buf[...] = jnp.where(mask, k, jnp.zeros_like(k))

    def scores(h, j, s_buf, k_buf):
        off, _ = window(h)
        q = qkv_ref[j * rows:(j + 1) * rows, pl.ds(off, WINDOW)]
        s_buf[...] = lax.dot_general(q, k_buf[...], NT, preferred_element_type=F32)

    mask_keys(0, k_bufs[0])
    scores(0, 0, s_bufs[0], k_bufs[0])

    def some_heads(i, carry):
        t = 0
        for u in range(unroll):
            h = i * unroll + u
            off, mask = window(h)
            for j in range(blocks):
                if j + 1 < blocks:
                    scores(h, j + 1, s_bufs[(t + 1) % 2], k_bufs[u % 2])
                else:
                    after = jnp.minimum(h + 1, heads - 1)
                    mask_keys(after, k_bufs[(u + 1) % 2])
                    scores(after, 0, s_bufs[(t + 1) % 2], k_bufs[(u + 1) % 2])
                s = s_bufs[t % 2][...]
                peak = jnp.max(s, axis=-1, keepdims=True)
                p = jnp.exp2((s - peak) * score_scale)
                total = jnp.sum(p, axis=-1, keepdims=True)
                v = qkv_ref[:, pl.ds(pl.multiple_of(2 * d + off, 128), WINDOW)]
                o = jnp.dot(p.astype(BF16), v, preferred_element_type=F32)
                o = (o * (1.0 / total)).astype(BF16)
                place = (pl.ds(j * rows, rows), pl.ds(off, WINDOW))
                out_ref[place] = jnp.where(mask, o, out_ref[place])
                t += 1
        return carry

    lax.fori_loop(0, heads // unroll, some_heads, 0)


def attn_call(qkv, images, heads, head_dim, rows=512, unroll=2):
    m, n = qkv.shape
    seq = m // images
    d = heads * head_dim
    return pl.pallas_call(
        functools.partial(attn_kernel, heads=heads, head_dim=head_dim, rows=rows, unroll=unroll),
        grid=(images,),
        name="attn",
        in_specs=[pl.BlockSpec((seq, n), lambda i: (i, 0))],
        out_specs=pl.BlockSpec((seq, d), lambda i: (i, 0)),
        out_shape=jax.ShapeDtypeStruct((m, d), BF16),
        scratch_shapes=[pltpu.VMEM((rows, seq), F32)] * 2 + [pltpu.VMEM((seq, WINDOW), BF16)] * 2,
        compiler_params=pltpu.CompilerParams(vmem_limit_bytes=VMEM_LIMIT),
        cost_estimate=pl.CostEstimate(flops=8 * images * heads * seq * seq * 256, bytes_accessed=2 * (m * n + m * d), transcendentals=images * heads * seq * seq),
    )(qkv)


def proj_kernel(o_ref, h_ref, wo_ref, bo_ref, out_ref, *, layer):
    proj = jnp.dot(o_ref[...], wo_ref[...], preferred_element_type=F32) + bo_ref[layer:layer + 1, :]
    out_ref[...] = (h_ref[...].astype(F32) + proj).astype(BF16)


def proj_call(layer, o, h, wo, bo, rows=512):
    m, d = o.shape
    block = pl.BlockSpec((rows, d), lambda i: (i, 0))
    return pl.pallas_call(
        functools.partial(proj_kernel, layer=layer),
        grid=(m // rows,),
        name="proj",
        in_specs=[block, block, layer_of(layer, (d, d)), whole(bo.shape)],
        out_specs=block,
        out_shape=jax.ShapeDtypeStruct((m, d), BF16),
        compiler_params=pltpu.CompilerParams(vmem_limit_bytes=VMEM_LIMIT),
        cost_estimate=pl.CostEstimate(flops=2 * m * d * d, bytes_accessed=2 * (3 * m * d + d * d), transcendentals=0),
    )(o, h, wo, bo)


def mlp_kernel(*refs, layer, cols):
    mid_ref, gain_ref, shift_ref, wu_ref, bu_ref, wd_ref, bd_ref = refs[:7]
    out_ref, act_ref = refs[-2:]
    row = slice(layer, layer + 1)
    f = wu_ref.shape[0]
    normed = layer_norm(mid_ref[...], gain_ref[row, :], shift_ref[row, :])
    for c in range(0, f, cols):
        w = min(cols, f - c)
        up = lax.dot_general(normed, wu_ref[c:c + w, :], NT, preferred_element_type=F32) + bu_ref[row, c:c + w]
        act_ref[:, c:c + w] = jax.nn.gelu(up, approximate=True).astype(BF16)
    down = jnp.dot(act_ref[...], wd_ref[...], preferred_element_type=F32) + bd_ref[row, :]
    out_ref[...] = (mid_ref[...].astype(F32) + down).astype(BF16)


def mlp_call(layer, mid, gain, shift, wu, bu, wd, bd, rows=256, cols=512, total=None, start=0, into=None):
    m, d = mid.shape
    f = wu.shape[1]
    total = m if total is None else total
    first = start // rows
    args = [mid, gain, shift, wu, bu, wd, bd]
    specs = [pl.BlockSpec((rows, d), lambda i: (i, 0)), whole(gain.shape), whole(shift.shape), layer_of(layer, (f, d)), whole(bu.shape), layer_of(layer, (f, d)), whole(bd.shape)]
    if into is not None:
        args.append(into)
        specs.append(pl.BlockSpec(memory_space=pl.ANY))
    return pl.pallas_call(
        functools.partial(mlp_kernel, layer=layer, cols=cols),
        grid=(m // rows,),
        name="mlp",
        in_specs=specs,
        out_specs=pl.BlockSpec((rows, d), lambda i: (first + i, 0)),
        out_shape=jax.ShapeDtypeStruct((total, d), BF16),
        scratch_shapes=[pltpu.VMEM((rows, f), BF16)],
        input_output_aliases={7: 0} if into is not None else {},
        compiler_params=pltpu.CompilerParams(vmem_limit_bytes=VMEM_LIMIT),
        cost_estimate=pl.CostEstimate(flops=4 * m * d * f, bytes_accessed=4 * (m * d + f * d), transcendentals=m * f),
    )(*args)


def solution(mesh):
    token_spec = P('dp', 'sp', None)
    group = mesh.shape['sp']

    def device_step(image_tokens, ln1_gain, ln1_shift, w_qkv, b_qkv, w_out, b_out, ln2_gain, ln2_shift, w_up, b_up, w_down, b_down):
        images, tokens, d = image_tokens.shape
        layers, _, _, heads, head_dim = w_qkv.shape
        w_qkv_t = jnp.transpose(w_qkv, (0, 2, 3, 4, 1)).reshape(layers, 3 * d, d)
        w_up_t = jnp.transpose(w_up, (0, 2, 1))
        w_o = w_out.reshape(layers, d, d)
        b_in = b_qkv.reshape(layers, 3 * d)
        rounds = images // group
        part = group * tokens

        def exchange(rows):
            blocks = rows.reshape(group, tokens, rows.shape[-1])
            return lax.all_to_all(blocks, 'sp', 0, 0, tiled=True).reshape(part, rows.shape[-1])

        def qkv(l, h):
            return qkv_call(l, h, ln1_gain, ln1_shift, w_qkv_t, b_in)

        def mlp(l, mid, **kw):
            return mlp_call(l, mid, ln2_gain, ln2_shift, w_up_t, b_up, w_down, b_down, **kw)

        own = image_tokens.reshape(rounds, part, d)
        mids = []
        for r in range(rounds):
            h = exchange(own[r])
            x = qkv(0, h) if r == 0 else exchange(qkv(0, own[r]))
            for l in range(layers):
                if l:
                    x = qkv(l, h)
                o = attn_call(x, 1, heads, head_dim)
                mid = proj_call(l, o, h, w_o, b_out)
                if l < layers - 1:
                    h = mlp(l, mid)
            mids.append(exchange(mid))
        out = None
        for r in range(rounds):
            out = mlp(layers - 1, mids[r], total=rounds * part, start=r * part, into=out)
        return out.reshape(images, tokens, d)

    return jax.shard_map(device_step, mesh=mesh, in_specs=(token_spec,) + (P(),) * 12, out_specs=token_spec, check_vma=False)
```

```python
import functools
import math

import jax
import jax.numpy as jnp
from jax import lax
from jax.experimental import pallas as pl
from jax.experimental.pallas import tpu as pltpu
from jax.sharding import PartitionSpec as P

LN_EPS = 1e-6
BF16 = jnp.bfloat16
F32 = jnp.float32
NT = (((1,), (1,)), ((), ()))
VMEM_LIMIT = 63 << 20
CHUNK = 512
PIECES = 3
ROWS = 256
WINDOW = 256


def layer_norm(values, gain, shift):
    values = values.astype(F32)
    centred = values - jnp.mean(values, axis=-1, keepdims=True)
    var = jnp.mean(centred * centred, axis=-1, keepdims=True)
    return (centred * lax.rsqrt(var + LN_EPS) * gain + shift).astype(BF16)


def whole(shape):
    return pl.BlockSpec(shape, lambda i: (0,) * len(shape), pipeline_mode=pl.Buffered(1))


def layer_of(layer, shape):
    return pl.BlockSpec((None,) + shape, lambda i: (layer,) + (0,) * len(shape), pipeline_mode=pl.Buffered(1))


def project(normed_ref, w_ref, bias_row, out_ref, rows=512, cols=256):
    m, n_out = normed_ref.shape[0], w_ref.shape[0]

    def step(i, carry):
        at = pl.ds(pl.multiple_of(i * rows, rows), rows)
        normed = normed_ref[at, :]
        for c in range(0, n_out, cols):
            w = min(cols, n_out - c)
            y = lax.dot_general(normed, w_ref[c:c + w, :], NT, preferred_element_type=F32)
            out_ref[at, c:c + w] = (y + bias_row[:, c:c + w]).astype(BF16)
        return carry

    lax.fori_loop(0, m // rows, step, 0)


def qkv_kernel(x_ref, gain_ref, shift_ref, w_ref, bias_ref, out_ref, *, cols):
    normed = layer_norm(x_ref[...], gain_ref[0:1, :], shift_ref[0:1, :])
    n_out = w_ref.shape[0]
    for c in range(0, n_out, cols):
        w = min(cols, n_out - c)
        y = lax.dot_general(normed, w_ref[c:c + w, :], NT, preferred_element_type=F32)
        out_ref[:, c:c + w] = (y + bias_ref[0:1, c:c + w]).astype(BF16)
    out_ref[:, n_out:] = x_ref[...]


def qkv_call(x, start, m, gain, shift, w, bias, rows=512, cols=256):
    d = x.shape[1]
    n = w.shape[1]
    first = start // rows
    return pl.pallas_call(
        functools.partial(qkv_kernel, cols=cols),
        grid=(m // rows,),
        name="qkv",
        in_specs=[pl.BlockSpec((rows, d), lambda i: (first + i, 0)), whole(gain.shape), whole(shift.shape), layer_of(0, (n, d)), whole(bias.shape)],
        out_specs=pl.BlockSpec((rows, n + d), lambda i: (i, 0)),
        out_shape=jax.ShapeDtypeStruct((m, n + d), BF16),
        compiler_params=pltpu.CompilerParams(vmem_limit_bytes=VMEM_LIMIT),
        cost_estimate=pl.CostEstimate(flops=2 * m * d * n, bytes_accessed=2 * (2 * m * d + n * d + m * n), transcendentals=0),
    )(x, gain, shift, w, bias)


def attend(qkv_ref, out_ref, s_bufs, k_bufs, *, heads, head_dim, rows=512, unroll=2):
    seq = qkv_ref.shape[0]
    d = heads * head_dim
    blocks = seq // rows
    score_scale = (head_dim ** -0.5) * math.log2(math.e)

    def window(h):
        low = h * head_dim
        off = pl.multiple_of(jnp.minimum(low // 128, d // 128 - 2) * 128, 128)
        low = low - off
        lane = lax.broadcasted_iota(jnp.int32, (1, WINDOW), 1)
        return off, (lane >= low) & (lane < low + head_dim)

    def mask_keys(h, k_buf):
        off, mask = window(h)
        k = qkv_ref[:, pl.ds(pl.multiple_of(d + off, 128), WINDOW)]
        k_buf[...] = jnp.where(mask, k, jnp.zeros_like(k))

    def scores(h, j, s_buf, k_buf):
        off, _ = window(h)
        q = qkv_ref[j * rows:(j + 1) * rows, pl.ds(off, WINDOW)]
        s_buf[...] = lax.dot_general(q, k_buf[...], NT, preferred_element_type=F32)

    mask_keys(0, k_bufs[0])
    scores(0, 0, s_bufs[0], k_bufs[0])

    def some_heads(i, carry):
        t = 0
        for u in range(unroll):
            h = i * unroll + u
            off, mask = window(h)
            for j in range(blocks):
                if j + 1 < blocks:
                    scores(h, j + 1, s_bufs[(t + 1) % 2], k_bufs[u % 2])
                else:
                    after = jnp.minimum(h + 1, heads - 1)
                    mask_keys(after, k_bufs[(u + 1) % 2])
                    scores(after, 0, s_bufs[(t + 1) % 2], k_bufs[(u + 1) % 2])
                s = s_bufs[t % 2][...]
                peak = jnp.max(s, axis=-1, keepdims=True)
                p = jnp.exp2((s - peak) * score_scale)
                total = jnp.sum(p, axis=-1, keepdims=True)
                v = qkv_ref[:, pl.ds(pl.multiple_of(2 * d + off, 128), WINDOW)]
                o = jnp.dot(p.astype(BF16), v, preferred_element_type=F32)
                o = (o * (1.0 / total)).astype(BF16)
                place = (pl.ds(j * rows, rows), pl.ds(off, WINDOW))
                out_ref[place] = jnp.where(mask, o, out_ref[place])
                t += 1
        return carry

    lax.fori_loop(0, heads // unroll, some_heads, 0)


class Chunks:
    def __init__(self, hbm, vmem, sem, f):
        per = -(-f // (PIECES * CHUNK)) * CHUNK
        self.hbm, self.vmem, self.sem = hbm, vmem, sem
        self.bounds = [(p, min(per, f - p)) for p in range(0, f, per)]

    def copy(self, l, p):
        at = pl.ds(*self.bounds[p])
        return pltpu.make_async_copy(self.hbm.at[l, at, :], self.vmem.at[at, :], self.sem.at[p])

    def start(self, l):
        for p in range(len(self.bounds)):
            self.copy(l, p).start()

    def wait(self, l):
        for p in range(len(self.bounds)):
            self.copy(l, p).wait()


def mlp_block(l, at, h_ref, up, down, bu_ref, bd_ref, gain_ref, shift_ref, act_ref, streamed=False):
    row = pl.ds(l, 1)
    f = act_ref.shape[1]
    normed = layer_norm(h_ref[at, :], gain_ref[row, :], shift_ref[row, :])
    for p, (start, size) in enumerate(up.bounds):
        if streamed:
            up.copy(l, p).wait()
        for c in range(start, start + size, CHUNK):
            w = min(CHUNK, f - c)
            x = lax.dot_general(normed, up.vmem[c:c + w, :], NT, preferred_element_type=F32) + bu_ref[row, c:c + w]
            act_ref[:, c:c + w] = jax.nn.gelu(x, approximate=True).astype(BF16)
    y = h_ref[at, :].astype(F32) + bd_ref[row, :]
    if not streamed:
        return y + jnp.dot(act_ref[...], down.vmem[...], preferred_element_type=F32)
    for p, (start, size) in enumerate(down.bounds):
        down.copy(l, p).wait()
        y = y + jnp.dot(act_ref[:, start:start + size], down.vmem[start:start + size, :], preferred_element_type=F32)
    return y


def layers_kernel(*refs, projected, layers, heads, head_dim):
    (x_hbm, g1, s1, wi_hbm, bi, wo_hbm, bo, g2, s2, wu_hbm, bu, wd_hbm, bd, out_hbm,
     h, qkv, o, s_a, s_b, k_a, k_b, act, wi, wo, wu, wd, sem, up_sem, down_sem) = refs
    d = heads * head_dim
    f = wu.shape[0]
    up, down = Chunks(wu_hbm, wu, up_sem, f), Chunks(wd_hbm, wd, down_sem, f)
    wi_copy = lambda l: pltpu.make_async_copy(wi_hbm.at[l], wi, sem.at[0])
    wo_copy = lambda l: pltpu.make_async_copy(wo_hbm.at[l], wo, sem.at[1])
    if projected:
        h_copy = pltpu.make_async_copy(x_hbm.at[:, 3 * d:], h, sem.at[2])
        qkv_copy = pltpu.make_async_copy(x_hbm.at[:, :3 * d], qkv, sem.at[3])
        qkv_copy.start()
        h_copy.start()
        wo_copy(0).start()
        up.start(0)
        down.start(0)
        wi_copy(1).start()
        h_copy.wait()
        qkv_copy.wait()
    else:
        h_copy = pltpu.make_async_copy(x_hbm, h, sem.at[2])
        h_copy.start()
        wi_copy(0).start()
        wo_copy(0).start()
        up.start(0)
        down.start(0)
        h_copy.wait()
        o[...] = layer_norm(h[...], g1[0:1, :], s1[0:1, :])

    def layer(l, carry):
        def make_qkv():
            wi_copy(l).wait()
            project(o, wi, bi.at[pl.ds(l, 1), :], qkv)

            @pl.when(l + 1 < layers)
            def _():
                wi_copy(l + 1).start()

        if projected:
            pl.when(l > 0)(make_qkv)
        else:
            make_qkv()
        attend(qkv, o, (s_a, s_b), (k_a, k_b), heads=heads, head_dim=head_dim)
        wo_copy(l).wait()

        def out_proj(i, c):
            at = pl.ds(pl.multiple_of(i * 512, 512), 512)
            y = jnp.dot(o[at, :], wo[...], preferred_element_type=F32) + bo[pl.ds(l, 1), :]
            h[at, :] = (h[at, :].astype(F32) + y).astype(BF16)
            return c

        lax.fori_loop(0, h.shape[0] // 512, out_proj, 0)

        @pl.when(l + 1 < layers)
        def _():
            wo_copy(l + 1).start()

            def finish(at, y):
                y = y.astype(BF16)
                h[at, :] = y
                o[at, :] = layer_norm(y, g1[pl.ds(l + 1, 1), :], s1[pl.ds(l + 1, 1), :])

            up.wait(l)
            down.wait(l)

            def block(i, c):
                at = pl.ds(pl.multiple_of(i * ROWS, ROWS), ROWS)
                finish(at, mlp_block(l, at, h, up, down, bu, bd, g2, s2, act))
                return c

            lax.fori_loop(0, h.shape[0] // ROWS, block, 0)

            @pl.when(l + 2 < layers)
            def _():
                up.start(l + 1)
                down.start(l + 1)

        return carry

    lax.fori_loop(0, layers, layer, 0)
    out = pltpu.make_async_copy(h, out_hbm, sem.at[2])
    out.start()
    out.wait()


def layers_call(x, projected, params, heads, head_dim):
    g1, s1, wi, bi, wo, bo, g2, s2, wu, bu, wd, bd = params
    m = x.shape[0]
    layers, n, d = wi.shape
    f = wu.shape[1]
    any_spec = pl.BlockSpec(memory_space=pl.ANY)
    vmem = pl.BlockSpec(memory_space=pltpu.VMEM)
    flops = layers * m * (2 * d * (n + d) + 4 * m * d * 3) + (layers - 1) * m * 4 * d * f
    return pl.pallas_call(
        functools.partial(layers_kernel, projected=projected, layers=layers, heads=heads, head_dim=head_dim),
        name="layers",
        in_specs=[any_spec, vmem, vmem, any_spec, vmem, any_spec, vmem, vmem, vmem, any_spec, vmem, any_spec, vmem],
        out_specs=any_spec,
        out_shape=jax.ShapeDtypeStruct((m, d), BF16),
        scratch_shapes=[
            pltpu.VMEM((m, d), BF16), pltpu.VMEM((m, n), BF16), pltpu.VMEM((m, d), BF16),
            pltpu.VMEM((512, m), F32), pltpu.VMEM((512, m), F32), pltpu.VMEM((m, WINDOW), BF16), pltpu.VMEM((m, WINDOW), BF16),
            pltpu.VMEM((ROWS, f), BF16),
            pltpu.VMEM((n, d), BF16), pltpu.VMEM((d, d), BF16), pltpu.VMEM((f, d), BF16), pltpu.VMEM((f, d), BF16),
            pltpu.SemaphoreType.DMA((4,)), pltpu.SemaphoreType.DMA((PIECES,)), pltpu.SemaphoreType.DMA((PIECES,)),
        ],
        compiler_params=pltpu.CompilerParams(vmem_limit_bytes=VMEM_LIMIT),
        cost_estimate=pl.CostEstimate(flops=flops, bytes_accessed=2 * layers * d * (n + d + 2 * f), transcendentals=layers * heads * m * m),
    )(x, g1, s1, wi, bi, wo, bo, g2, s2, wu, bu, wd, bd)


def last_mlp_kernel(*refs, layer, start):
    m_hbm, g2, s2, wu_hbm, bu, wd_hbm, bd = refs[:7]
    out_hbm, h, out, act, wu, wd, h_sem, out_sem, up_sem, down_sem = refs[-10:]
    f = wu.shape[0]
    steps = h.shape[0] // ROWS
    up, down = Chunks(wu_hbm, wu, up_sem, f), Chunks(wd_hbm, wd, down_sem, f)
    first = pl.ds(0, ROWS)
    rest = pl.ds(ROWS, h.shape[0] - ROWS)
    copies = [pltpu.make_async_copy(m_hbm.at[at, :], h.at[at, :], h_sem.at[i]) for i, at in enumerate((first, rest))]
    copies[0].start()
    up.start(layer)
    copies[1].start()
    down.start(layer)

    def finish(i, streamed):
        at = pl.ds(pl.multiple_of(i * ROWS, ROWS), ROWS)
        y = mlp_block(layer, at, h, up, down, bu, bd, g2, s2, act, streamed)
        out[at, :] = y.astype(BF16)

    def write(i):
        at = pl.multiple_of(i * ROWS, ROWS)
        return pltpu.make_async_copy(out.at[pl.ds(at, ROWS), :], out_hbm.at[pl.ds(start + at, ROWS), :], out_sem.at[i])

    copies[0].wait()
    finish(0, True)
    write(0).start()
    copies[1].wait()

    def step(i, carry):
        finish(i, False)
        write(i).start()
        return carry

    lax.fori_loop(1, steps, step, 0)
    for i in range(steps):
        write(i).wait()


def last_mlp_call(layer, mid, params, total, start, into):
    g1, s1, wi, bi, wo, bo, g2, s2, wu, bu, wd, bd = params
    m, d = mid.shape
    f = wu.shape[1]
    any_spec = pl.BlockSpec(memory_space=pl.ANY)
    vmem = pl.BlockSpec(memory_space=pltpu.VMEM)
    args = [mid, g2, s2, wu, bu, wd, bd]
    specs = [any_spec, vmem, vmem, any_spec, vmem, any_spec, vmem]
    if into is not None:
        args.append(into)
        specs.append(any_spec)
    return pl.pallas_call(
        functools.partial(last_mlp_kernel, layer=layer, start=start),
        name="last_mlp",
        in_specs=specs,
        out_specs=any_spec,
        out_shape=jax.ShapeDtypeStruct((total, d), BF16),
        scratch_shapes=[
            pltpu.VMEM((m, d), BF16), pltpu.VMEM((m, d), BF16), pltpu.VMEM((ROWS, f), BF16), pltpu.VMEM((f, d), BF16), pltpu.VMEM((f, d), BF16),
            pltpu.SemaphoreType.DMA((2,)), pltpu.SemaphoreType.DMA((m // ROWS,)), pltpu.SemaphoreType.DMA((PIECES,)), pltpu.SemaphoreType.DMA((PIECES,)),
        ],
        input_output_aliases={7: 0} if into is not None else {},
        compiler_params=pltpu.CompilerParams(vmem_limit_bytes=VMEM_LIMIT),
        cost_estimate=pl.CostEstimate(flops=4 * m * d * f, bytes_accessed=4 * (m * d + f * d), transcendentals=m * f),
    )(*args)


def solution(mesh):
    token_spec = P('dp', 'sp', None)
    group = mesh.shape['sp']

    def device_step(image_tokens, ln1_gain, ln1_shift, w_qkv, b_qkv, w_out, b_out, ln2_gain, ln2_shift, w_up, b_up, w_down, b_down):
        images, tokens, d = image_tokens.shape
        layers, _, _, heads, head_dim = w_qkv.shape
        w_qkv_t = jnp.transpose(w_qkv, (0, 2, 3, 4, 1)).reshape(layers, 3 * d, d)
        params = (ln1_gain, ln1_shift, w_qkv_t, b_qkv.reshape(layers, 3 * d), w_out.reshape(layers, d, d), b_out,
                  ln2_gain, ln2_shift, jnp.transpose(w_up, (0, 2, 1)), b_up, w_down, b_down)
        rounds = images // group
        part = group * tokens

        def exchange(rows):
            blocks = rows.reshape(group, tokens, rows.shape[-1])
            return lax.all_to_all(blocks, 'sp', 0, 0, tiled=True).reshape(part, rows.shape[-1])

        own = image_tokens.reshape(rounds * part, d)
        moved = [exchange(own[:part])]
        for r in range(1, rounds):
            moved.append(exchange(qkv_call(own, r * part, part, ln1_gain, ln1_shift, w_qkv_t, params[3])))
        mids = [exchange(layers_call(moved[r], r > 0, params, heads, head_dim)) for r in range(rounds)]
        out = None
        for r in range(rounds):
            out = last_mlp_call(layers - 1, mids[r], params, rounds * part, r * part, out)
        return out.reshape(images, tokens, d)

    return jax.shard_map(device_step, mesh=mesh, in_specs=(token_spec,) + (P(),) * 12, out_specs=token_spec, check_vma=False)
```

```python
import functools
import math

import jax
import jax.numpy as jnp
from jax import lax
from jax.experimental import pallas as pl
from jax.experimental.pallas import tpu as pltpu
from jax.sharding import PartitionSpec as P

LN_EPS = 1e-6
BF16 = jnp.bfloat16
F32 = jnp.float32
NT = (((1,), (1,)), ((), ()))
VMEM_LIMIT = 63 << 20
CHUNK = 512
PIECES = 3
ROWS = 256
AHEAD = 2
WINDOW = 256


def layer_norm(values, gain, shift):
    values = values.astype(F32)
    centred = values - jnp.mean(values, axis=-1, keepdims=True)
    var = jnp.mean(centred * centred, axis=-1, keepdims=True)
    return (centred * lax.rsqrt(var + LN_EPS) * gain + shift).astype(BF16)


def whole(shape):
    return pl.BlockSpec(shape, lambda i: (0,) * len(shape), pipeline_mode=pl.Buffered(1))


def layer_of(layer, shape):
    return pl.BlockSpec((None,) + shape, lambda i: (layer,) + (0,) * len(shape), pipeline_mode=pl.Buffered(1))


def project(normed_ref, w_ref, bias_row, out_ref, rows=512, cols=256):
    m, n_out = normed_ref.shape[0], w_ref.shape[0]

    def step(i, carry):
        at = pl.ds(pl.multiple_of(i * rows, rows), rows)
        normed = normed_ref[at, :]
        for c in range(0, n_out, cols):
            w = min(cols, n_out - c)
            y = lax.dot_general(normed, w_ref[c:c + w, :], NT, preferred_element_type=F32)
            out_ref[at, c:c + w] = (y + bias_row[:, c:c + w]).astype(BF16)
        return carry

    lax.fori_loop(0, m // rows, step, 0)


def qkv_kernel(x_ref, gain_ref, shift_ref, w_ref, bias_ref, out_ref, *, cols):
    normed = layer_norm(x_ref[...], gain_ref[0:1, :], shift_ref[0:1, :])
    n_out = w_ref.shape[0]
    for c in range(0, n_out, cols):
        w = min(cols, n_out - c)
        y = lax.dot_general(normed, w_ref[c:c + w, :], NT, preferred_element_type=F32)
        out_ref[:, c:c + w] = (y + bias_ref[0:1, c:c + w]).astype(BF16)
    out_ref[:, n_out:] = x_ref[...]


def qkv_call(x, start, m, gain, shift, w, bias, rows=512, cols=256):
    d = x.shape[1]
    n = w.shape[1]
    first = start // rows
    return pl.pallas_call(
        functools.partial(qkv_kernel, cols=cols),
        grid=(m // rows,),
        name="qkv",
        in_specs=[pl.BlockSpec((rows, d), lambda i: (first + i, 0)), whole(gain.shape), whole(shift.shape), layer_of(0, (n, d)), whole(bias.shape)],
        out_specs=pl.BlockSpec((rows, n + d), lambda i: (i, 0)),
        out_shape=jax.ShapeDtypeStruct((m, n + d), BF16),
        compiler_params=pltpu.CompilerParams(vmem_limit_bytes=VMEM_LIMIT),
        cost_estimate=pl.CostEstimate(flops=2 * m * d * n, bytes_accessed=2 * (2 * m * d + n * d + m * n), transcendentals=0),
    )(x, gain, shift, w, bias)


def attend(qkv_ref, out_ref, s_bufs, k_bufs, *, heads, head_dim, rows=512, unroll=2):
    seq = qkv_ref.shape[0]
    d = heads * head_dim
    blocks = seq // rows
    score_scale = (head_dim ** -0.5) * math.log2(math.e)

    def window(h):
        low = h * head_dim
        off = pl.multiple_of(jnp.minimum(low // 128, d // 128 - 2) * 128, 128)
        low = low - off
        lane = lax.broadcasted_iota(jnp.int32, (1, WINDOW), 1)
        return off, (lane >= low) & (lane < low + head_dim)

    def mask_keys(h, k_buf):
        off, mask = window(h)
        k = qkv_ref[:, pl.ds(pl.multiple_of(d + off, 128), WINDOW)]
        k_buf[...] = jnp.where(mask, k, jnp.zeros_like(k))

    def scores(h, j, s_buf, k_buf):
        off, _ = window(h)
        q = qkv_ref[j * rows:(j + 1) * rows, pl.ds(off, WINDOW)]
        s_buf[...] = lax.dot_general(q, k_buf[...], NT, preferred_element_type=F32)

    mask_keys(0, k_bufs[0])
    scores(0, 0, s_bufs[0], k_bufs[0])

    def some_heads(i, carry):
        t = 0
        for u in range(unroll):
            h = i * unroll + u
            off, mask = window(h)
            for j in range(blocks):
                if j + 1 < blocks:
                    scores(h, j + 1, s_bufs[(t + 1) % 2], k_bufs[u % 2])
                else:
                    after = jnp.minimum(h + 1, heads - 1)
                    mask_keys(after, k_bufs[(u + 1) % 2])
                    scores(after, 0, s_bufs[(t + 1) % 2], k_bufs[(u + 1) % 2])
                s = s_bufs[t % 2][...]
                peak = jnp.max(s, axis=-1, keepdims=True)
                p = jnp.exp2((s - peak) * score_scale)
                total = jnp.sum(p, axis=-1, keepdims=True)
                v = qkv_ref[:, pl.ds(pl.multiple_of(2 * d + off, 128), WINDOW)]
                o = jnp.dot(p.astype(BF16), v, preferred_element_type=F32)
                o = (o * (1.0 / total)).astype(BF16)
                place = (pl.ds(j * rows, rows), pl.ds(off, WINDOW))
                out_ref[place] = jnp.where(mask, o, out_ref[place])
                t += 1
        return carry

    lax.fori_loop(0, heads // unroll, some_heads, 0)


class Chunks:
    def __init__(self, hbm, vmem, sem, f):
        per = -(-f // (PIECES * CHUNK)) * CHUNK
        self.hbm, self.vmem, self.sem = hbm, vmem, sem
        self.bounds = [(p, min(per, f - p)) for p in range(0, f, per)]

    def copy(self, l, p):
        at = pl.ds(*self.bounds[p])
        return pltpu.make_async_copy(self.hbm.at[l, at, :], self.vmem.at[at, :], self.sem.at[p])

    def start(self, l):
        for p in range(len(self.bounds)):
            self.copy(l, p).start()

    def wait(self, l):
        for p in range(len(self.bounds)):
            self.copy(l, p).wait()


def mlp_block(l, at, h_ref, up, down, bu_ref, bd_ref, gain_ref, shift_ref, act_ref, streamed=False):
    row = pl.ds(l, 1)
    f = act_ref.shape[1]
    normed = layer_norm(h_ref[at, :], gain_ref[row, :], shift_ref[row, :])
    pieces = [(w, p) for w in (up, down) for p in range(len(w.bounds))]

    def arrive(k):
        w, p = pieces[k]
        w.copy(l, p).wait()
        if k + AHEAD < len(pieces):
            w, p = pieces[k + AHEAD]
            w.copy(l, p).start()

    for p, (start, size) in enumerate(up.bounds):
        if streamed:
            arrive(p)
        for c in range(start, start + size, CHUNK):
            w = min(CHUNK, f - c)
            x = lax.dot_general(normed, up.vmem[c:c + w, :], NT, preferred_element_type=F32) + bu_ref[row, c:c + w]
            act_ref[:, c:c + w] = jax.nn.gelu(x, approximate=True).astype(BF16)
    y = h_ref[at, :].astype(F32) + bd_ref[row, :]
    if not streamed:
        return y + jnp.dot(act_ref[...], down.vmem[...], preferred_element_type=F32)
    for p, (start, size) in enumerate(down.bounds):
        arrive(len(up.bounds) + p)
        y = y + jnp.dot(act_ref[:, start:start + size], down.vmem[start:start + size, :], preferred_element_type=F32)
    return y


def layers_kernel(*refs, projected, layers, heads, head_dim):
    (x_hbm, g1, s1, wi_hbm, bi, wo_hbm, bo, g2, s2, wu_hbm, bu, wd_hbm, bd, out_hbm,
     h, qkv, o, s_a, s_b, k_a, k_b, act, wi, wo, wu, wd, sem, up_sem, down_sem) = refs
    d = heads * head_dim
    f = wu.shape[0]
    up, down = Chunks(wu_hbm, wu, up_sem, f), Chunks(wd_hbm, wd, down_sem, f)
    wi_copy = lambda l: pltpu.make_async_copy(wi_hbm.at[l], wi, sem.at[0])
    wo_copy = lambda l: pltpu.make_async_copy(wo_hbm.at[l], wo, sem.at[1])
    if projected:
        h_copy = pltpu.make_async_copy(x_hbm.at[:, 3 * d:], h, sem.at[2])
        qkv_copy = pltpu.make_async_copy(x_hbm.at[:, :3 * d], qkv, sem.at[3])
        qkv_copy.start()
        qkv_copy.wait()
        h_copy.start()
        wo_copy(0).start()
        up.start(0)
        down.start(0)
        wi_copy(1).start()
    else:
        h_copy = pltpu.make_async_copy(x_hbm, h, sem.at[2])
        h_copy.start()
        wi_copy(0).start()
        h_copy.wait()
        o[...] = layer_norm(h[...], g1[0:1, :], s1[0:1, :])

    def layer(l, carry):
        def make_qkv():
            wi_copy(l).wait()
            if not projected:

                @pl.when(l == 0)
                def _():
                    wo_copy(0).start()
                    up.start(0)
                    down.start(0)

            project(o, wi, bi.at[pl.ds(l, 1), :], qkv)

            @pl.when(l + 1 < layers)
            def _():
                wi_copy(l + 1).start()

        if projected:
            pl.when(l > 0)(make_qkv)
        else:
            make_qkv()
        attend(qkv, o, (s_a, s_b), (k_a, k_b), heads=heads, head_dim=head_dim, unroll=4 if projected else 2)
        wo_copy(l).wait()
        if projected:
            pl.when(l == 0)(h_copy.wait)

        def out_proj(i, c):
            at = pl.ds(pl.multiple_of(i * 512, 512), 512)
            y = jnp.dot(o[at, :], wo[...], preferred_element_type=F32) + bo[pl.ds(l, 1), :]
            h[at, :] = (h[at, :].astype(F32) + y).astype(BF16)
            return c

        lax.fori_loop(0, h.shape[0] // 512, out_proj, 0)

        @pl.when(l + 1 < layers)
        def _():
            wo_copy(l + 1).start()

            def finish(at, y):
                y = y.astype(BF16)
                h[at, :] = y
                o[at, :] = layer_norm(y, g1[pl.ds(l + 1, 1), :], s1[pl.ds(l + 1, 1), :])

            up.wait(l)
            down.wait(l)

            def block(i, c):
                at = pl.ds(pl.multiple_of(i * ROWS, ROWS), ROWS)
                finish(at, mlp_block(l, at, h, up, down, bu, bd, g2, s2, act))
                return c

            lax.fori_loop(0, h.shape[0] // ROWS, block, 0)

            @pl.when(l + 2 < layers)
            def _():
                up.start(l + 1)
                down.start(l + 1)

        return carry

    lax.fori_loop(0, layers, layer, 0)
    out = pltpu.make_async_copy(h, out_hbm, sem.at[2])
    out.start()
    out.wait()


def layers_call(x, projected, params, heads, head_dim):
    g1, s1, wi, bi, wo, bo, g2, s2, wu, bu, wd, bd = params
    m = x.shape[0]
    layers, n, d = wi.shape
    f = wu.shape[1]
    any_spec = pl.BlockSpec(memory_space=pl.ANY)
    vmem = pl.BlockSpec(memory_space=pltpu.VMEM)
    flops = layers * m * (2 * d * (n + d) + 4 * m * d * 3) + (layers - 1) * m * 4 * d * f
    return pl.pallas_call(
        functools.partial(layers_kernel, projected=projected, layers=layers, heads=heads, head_dim=head_dim),
        name="layers",
        in_specs=[any_spec, vmem, vmem, any_spec, vmem, any_spec, vmem, vmem, vmem, any_spec, vmem, any_spec, vmem],
        out_specs=any_spec,
        out_shape=jax.ShapeDtypeStruct((m, d), BF16),
        scratch_shapes=[
            pltpu.VMEM((m, d), BF16), pltpu.VMEM((m, n), BF16), pltpu.VMEM((m, d), BF16),
            pltpu.VMEM((512, m), F32), pltpu.VMEM((512, m), F32), pltpu.VMEM((m, WINDOW), BF16), pltpu.VMEM((m, WINDOW), BF16),
            pltpu.VMEM((ROWS, f), BF16),
            pltpu.VMEM((n, d), BF16), pltpu.VMEM((d, d), BF16), pltpu.VMEM((f, d), BF16), pltpu.VMEM((f, d), BF16),
            pltpu.SemaphoreType.DMA((4,)), pltpu.SemaphoreType.DMA((PIECES,)), pltpu.SemaphoreType.DMA((PIECES,)),
        ],
        compiler_params=pltpu.CompilerParams(vmem_limit_bytes=VMEM_LIMIT),
        cost_estimate=pl.CostEstimate(flops=flops, bytes_accessed=2 * layers * d * (n + d + 2 * f), transcendentals=layers * heads * m * m),
    )(x, g1, s1, wi, bi, wo, bo, g2, s2, wu, bu, wd, bd)


def last_mlp_kernel(*refs, layer, start):
    m_hbm, g2, s2, wu_hbm, bu, wd_hbm, bd = refs[:7]
    out_hbm, h, out, act, wu, wd, h_sem, out_sem, up_sem, down_sem = refs[-10:]
    f = wu.shape[0]
    steps = h.shape[0] // ROWS
    up, down = Chunks(wu_hbm, wu, up_sem, f), Chunks(wd_hbm, wd, down_sem, f)
    first = pl.ds(0, ROWS)
    rest = pl.ds(ROWS, h.shape[0] - ROWS)
    copies = [pltpu.make_async_copy(m_hbm.at[at, :], h.at[at, :], h_sem.at[i]) for i, at in enumerate((first, rest))]
    copies[0].start()
    for p in range(AHEAD):
        up.copy(layer, p).start()

    def finish(i, streamed):
        at = pl.ds(pl.multiple_of(i * ROWS, ROWS), ROWS)
        y = mlp_block(layer, at, h, up, down, bu, bd, g2, s2, act, streamed)
        out[at, :] = y.astype(BF16)

    def write(i):
        at = pl.multiple_of(i * ROWS, ROWS)
        return pltpu.make_async_copy(out.at[pl.ds(at, ROWS), :], out_hbm.at[pl.ds(start + at, ROWS), :], out_sem.at[i])

    copies[0].wait()
    copies[1].start()
    finish(0, True)
    write(0).start()
    copies[1].wait()

    def step(i, carry):
        finish(i, False)
        write(i).start()
        return carry

    lax.fori_loop(1, steps, step, 0)
    for i in range(steps):
        write(i).wait()


def last_mlp_call(layer, mid, params, total, start, into):
    g1, s1, wi, bi, wo, bo, g2, s2, wu, bu, wd, bd = params
    m, d = mid.shape
    f = wu.shape[1]
    any_spec = pl.BlockSpec(memory_space=pl.ANY)
    vmem = pl.BlockSpec(memory_space=pltpu.VMEM)
    args = [mid, g2, s2, wu, bu, wd, bd]
    specs = [any_spec, vmem, vmem, any_spec, vmem, any_spec, vmem]
    if into is not None:
        args.append(into)
        specs.append(any_spec)
    return pl.pallas_call(
        functools.partial(last_mlp_kernel, layer=layer, start=start),
        name="last_mlp",
        in_specs=specs,
        out_specs=any_spec,
        out_shape=jax.ShapeDtypeStruct((total, d), BF16),
        scratch_shapes=[
            pltpu.VMEM((m, d), BF16), pltpu.VMEM((m, d), BF16), pltpu.VMEM((ROWS, f), BF16), pltpu.VMEM((f, d), BF16), pltpu.VMEM((f, d), BF16),
            pltpu.SemaphoreType.DMA((2,)), pltpu.SemaphoreType.DMA((m // ROWS,)), pltpu.SemaphoreType.DMA((PIECES,)), pltpu.SemaphoreType.DMA((PIECES,)),
        ],
        input_output_aliases={7: 0} if into is not None else {},
        compiler_params=pltpu.CompilerParams(vmem_limit_bytes=VMEM_LIMIT),
        cost_estimate=pl.CostEstimate(flops=4 * m * d * f, bytes_accessed=4 * (m * d + f * d), transcendentals=m * f),
    )(*args)


def solution(mesh):
    token_spec = P('dp', 'sp', None)
    group = mesh.shape['sp']

    def device_step(image_tokens, ln1_gain, ln1_shift, w_qkv, b_qkv, w_out, b_out, ln2_gain, ln2_shift, w_up, b_up, w_down, b_down):
        images, tokens, d = image_tokens.shape
        layers, _, _, heads, head_dim = w_qkv.shape
        w_qkv_t = jnp.transpose(w_qkv, (0, 2, 3, 4, 1)).reshape(layers, 3 * d, d)
        params = (ln1_gain, ln1_shift, w_qkv_t, b_qkv.reshape(layers, 3 * d), w_out.reshape(layers, d, d), b_out,
                  ln2_gain, ln2_shift, jnp.transpose(w_up, (0, 2, 1)), b_up, w_down, b_down)
        rounds = images // group
        part = group * tokens

        def exchange(rows):
            blocks = rows.reshape(group, tokens, rows.shape[-1])
            return lax.all_to_all(blocks, 'sp', 0, 0, tiled=True).reshape(part, rows.shape[-1])

        own = image_tokens.reshape(rounds * part, d)
        moved = [exchange(own[:part])]
        for r in range(1, rounds):
            moved.append(exchange(qkv_call(own, r * part, part, ln1_gain, ln1_shift, w_qkv_t, params[3])))
        mids = [exchange(layers_call(moved[r], r > 0, params, heads, head_dim)) for r in range(rounds)]
        out = None
        for r in range(rounds):
            out = last_mlp_call(layers - 1, mids[r], params, rounds * part, r * part, out)
        return out.reshape(images, tokens, d)

    return jax.shard_map(device_step, mesh=mesh, in_specs=(token_spec,) + (P(),) * 12, out_specs=token_spec, check_vma=False)
```
